256 devices in a mesh: section: 16 (over x, y), expert: 16 (over z, core).
Axes of the slice: x: 4, y: 4, z: 8, core: 2. Of those that a mesh axis runs over, the one named last changes fastest.
Arguments:
- tokens: bfloat16 [8, 128, 2048], P(None, 'expert'), may hold values from -6 to 6
- norm_gain: float32 [8, 2048], replicated, may hold values from 0.1 to 1.9
- w_gate: bfloat16 [16, 2048, 14336], P('section', None, 'expert'), may hold values from -0.125 to 0.125
- w_up: bfloat16 [16, 2048, 14336], P('section', None, 'expert'), may hold values from -0.125 to 0.125
- w_down: bfloat16 [16, 14336, 2048], P('section', 'expert'), may hold values from -0.0625 to 0.0625
- expert_ids: int32 [8, 8, 128, 2], P(None, None, 'expert'), may hold values from 0 to 3, as said below
- slot_ids: int32 [8, 8, 128, 2], P(None, None, 'expert'), may hold values from 0 to 4, as said below
- dropped: int32 [8, 8, 128, 2], P(None, None, 'expert'), may hold values from 0 to 1, as said below
- gate_weights: float32 [8, 8, 128, 2], P(None, None, 'expert'), may hold values from 0.1 to 1
Outputs:
- states: bfloat16 [16, 8, 128, 2048], P('section', None, 'expert')
The draws below stay inside these ranges and needn't reach their ends.
Inputs may be any that keep to these rules, and one draw needn't show every extreme that they name: `expert_ids`: the two experts of a token differ. `slot_ids`: among the kept choices of the tokens of one index of expert that name one expert, the slots are 0, 1, ... up to their count less one, each once. At most 5 kept choices of the tokens of one index of expert name one expert, and a choice is dropped only where 5 kept choices of its index of expert name its expert; in each layer and micro-batch some expert receives exactly 5 kept choices from every index of expert.
All inputs are finite; a program needn't handle non-finite values.
Results may differ from the reference program's by a relative error of at most 0.025.
Values may be sent and summed in bfloat16 or wider, within the bound.
A program may use at most 64 MiB of HBM per device.

```python
import jax
import jax.numpy as jnp
from jax import lax

D = 2048
FF = 7168
EXPERTS = 4
TOK_DEV = 8
MICRO = 8
LOCAL = 2
SHARDS = 8
LAYERS = 8
TOKENS = 128
CAP = 5
N_EXPERT = 16


def routing_draw(key):
    folded = jax.random.fold_in(key, 7)
    subkeys = jax.random.split(folded, 5)
    blocks = LAYERS * MICRO * N_EXPERT
    hot_expert = jax.random.randint(subkeys[4], (LAYERS * MICRO,), 0, EXPERTS)
    hot_expert = jnp.repeat(hot_expert, N_EXPERT)[:, None]
    priority = jax.vmap(lambda subkey: jax.random.permutation(subkey, TOK_DEV))(jax.random.split(subkeys[2], blocks))
    random_pick = jax.random.randint(subkeys[0], (blocks, TOK_DEV), 0, EXPERTS)
    first_pick = jnp.where(priority < CAP, hot_expert, random_pick)
    offset = jax.random.randint(subkeys[1], (blocks, TOK_DEV), 1, EXPERTS)
    second = (first_pick + offset) % EXPERTS
    chosen = jnp.stack([first_pick, second], axis=-1).astype(jnp.int32)
    prio_pair = jnp.stack([priority * 2, priority * 2 + 1], axis=-1).reshape(blocks, 2 * TOK_DEV)
    flat_ids = chosen.reshape(blocks, 2 * TOK_DEV)
    same_expert = flat_ids[:, :, None] == flat_ids[:, None, :]
    earlier = prio_pair[:, None, :] < prio_pair[:, :, None]
    rank_vals = jnp.sum((same_expert & earlier).astype(jnp.int32), axis=-1)
    drop_flag = (rank_vals >= CAP).astype(jnp.int32)
    spare_slot = jax.random.randint(subkeys[3], (blocks, 2 * TOK_DEV), 0, CAP)
    slot_vals = jnp.where(drop_flag == 1, spare_slot, rank_vals).astype(jnp.int32)
    out_shape = (LAYERS, MICRO, TOKENS, 2)
    return (chosen.reshape(out_shape), slot_vals.reshape(out_shape), drop_flag.reshape(out_shape))


def draw_expert_ids(key, part):
    return routing_draw(key)[0]


def draw_slot_ids(key, part):
    return routing_draw(key)[1]


def draw_dropped(key, part):
    return routing_draw(key)[2]


def shard_levels(stream_key, extent, shards, least, high):
    def one(axis_at, shards_of):
        steps = jax.random.uniform(jax.random.fold_in(jax.random.fold_in(stream_key, 6), axis_at), (shards_of,), jnp.float32, least / len(shards), high / len(shards))
        return jnp.repeat(jnp.exp(steps), extent[axis_at] // shards_of).reshape((-1,) + (1,) * (len(extent) - axis_at - 1))

    level = one(*shards[0])
    for cut in shards[1:]:
        level = level * one(*cut)
    return level


def gaussian(rng, dims, deviation, reach, shards=(), held_as=jnp.bfloat16):
    result = deviation * jax.random.normal(rng, dims, jnp.float32)
    if shards:
        result = result * shard_levels(rng, dims, shards, -0.22, 0.18)
    return jnp.clip(result, -reach, reach).astype(held_as)


def setup_inputs(seed: int = 0) -> dict:
    keys = jax.random.split(jax.random.key(seed), 10)
    tokens = gaussian(keys[0], (MICRO, TOKENS, D), 1.0, 6.0, ((1, 16),))
    norm_gain = jnp.clip(1.0 + 0.18 * jax.random.normal(keys[1], (LAYERS, D), jnp.float32), 0.1, 1.9)
    w_gate = gaussian(keys[2], (2 * LAYERS, D, LOCAL * FF), D ** -0.5, 0.125, ((0, 16), (2, 16)))
    w_up = gaussian(keys[3], (2 * LAYERS, D, LOCAL * FF), D ** -0.5, 0.125, ((0, 16), (2, 16)))
    w_down = gaussian(keys[4], (2 * LAYERS, LOCAL * FF, D), FF ** -0.5, 0.0625, ((0, 16), (1, 16)))
    expert_ids = draw_expert_ids(jax.random.fold_in(keys[9], 71), 0)
    slot_ids = draw_slot_ids(jax.random.fold_in(keys[9], 71), 0)
    dropped = draw_dropped(jax.random.fold_in(keys[9], 71), 0)
    gate_weights = jnp.clip(0.1 + 0.9 * jax.random.uniform(keys[8], (LAYERS, MICRO, TOKENS, 2), jnp.float32) ** shard_levels(keys[8], (LAYERS, MICRO, TOKENS, 2), ((2, 16),), -0.2, 0.2), 0.1, 1.0)
    return dict(tokens=tokens, norm_gain=norm_gain, w_gate=w_gate, w_up=w_up, w_down=w_down, expert_ids=expert_ids, slot_ids=slot_ids, dropped=dropped, gate_weights=gate_weights)


def rms_norm(values, gain_row):
    wide_vals = values.astype(jnp.float32)
    inv_scale = lax.rsqrt(lax.optimization_barrier(jnp.mean(wide_vals * wide_vals, axis=-1, keepdims=True)) + 1e-05)
    return (wide_vals * inv_scale * gain_row).astype(jnp.bfloat16)

def expert_output(rows_in, gate_cols, up_cols, down_rows):
    row_count = rows_in.shape[0]
    gate_vals = jnp.dot(rows_in, gate_cols, preferred_element_type=jnp.float32)
    up_vals = jnp.dot(rows_in, up_cols, preferred_element_type=jnp.float32)
    hidden = (jax.nn.silu(gate_vals) * up_vals).astype(jnp.bfloat16)
    pieces = hidden.reshape(row_count, SHARDS, FF // SHARDS).astype(jnp.float32)
    blocks = down_rows.reshape(SHARDS, FF // SHARDS, D).astype(jnp.float32)
    partial_value = jnp.einsum('rsf,sfd->srd', pieces, blocks).astype(jnp.bfloat16)
    partial_value = lax.optimization_barrier(partial_value)
    return lax.optimization_barrier(jnp.sum(partial_value.astype(jnp.float32), axis=0)).astype(jnp.bfloat16)

def reference(tokens, norm_gain, w_gate, w_up, w_down, expert_ids, slot_ids, dropped, gate_weights):
    slot_limit = EXPERTS * N_EXPERT * CAP
    source = (jnp.arange(TOKENS, dtype=jnp.int32) // TOK_DEV)[:, None]
    gate_all = w_gate.reshape(LAYERS, 2, D, LOCAL * FF)
    up_all = w_up.reshape(LAYERS, 2, D, LOCAL * FF)
    down_all = w_down.reshape(LAYERS, 2, LOCAL * FF, D)

    def one_layer(state, layer_args):
        gain_row, gate_pair, up_pair, down_pair, route_all, slot_all, drop_all, weigh_all = layer_args

        def one_micro(pieces):
            current, route_now, slot_now, drop_now, weigh_now = pieces
            normed = rms_norm(current, gain_row)
            target = route_now * (N_EXPERT * CAP) + source * CAP + slot_now
            target = jnp.where(drop_now == 1, slot_limit, target).astype(jnp.int32)
            buffer = jnp.zeros((slot_limit, D), jnp.bfloat16)
            buffer = buffer.at[target[:, 0]].set(normed, mode='drop')
            buffer = buffer.at[target[:, 1]].set(normed, mode='drop')
            grouped = buffer.reshape(EXPERTS, N_EXPERT * CAP, D)
            outputs = []
            for expert_at in range(EXPERTS):
                half_index = expert_at // LOCAL
                inner_index = expert_at % LOCAL
                low = inner_index * FF
                high = (inner_index + 1) * FF
                outputs.append(expert_output(grouped[expert_at], gate_pair[half_index][:, low:high], up_pair[half_index][:, low:high], down_pair[half_index][low:high]))
            produced = jnp.concatenate(outputs, axis=0)
            clipped = jnp.minimum(target, slot_limit - 1).astype(jnp.int32)
            first_half = current.astype(jnp.float32)
            full_mix = current.astype(jnp.float32)
            for member in range(2):
                picked = produced[clipped[:, member]].astype(jnp.float32)
                weighted = weigh_now[:, member:member + 1] * picked
                kept_mask = drop_now[:, member:member + 1] == 0
                first_kept = kept_mask & (route_now[:, member:member + 1] < LOCAL)
                first_half = first_half + jnp.where(first_kept, weighted, 0.0)
                full_mix = full_mix + jnp.where(kept_mask, weighted, 0.0)
            return (first_half.astype(jnp.bfloat16), full_mix.astype(jnp.bfloat16))
        half_state, new_state = lax.map(one_micro, (state, route_all, slot_all, drop_all, weigh_all))
        return (new_state, jnp.stack([half_state, new_state]))
    final_state, paired = lax.scan(one_layer, tokens, (norm_gain, gate_all, up_all, down_all, expert_ids, slot_ids, dropped, gate_weights))
    return paired.reshape(2 * LAYERS, MICRO, TOKENS, D)
```

```python
import functools

import jax
import jax.numpy as jnp
from jax import lax
from jax.experimental import pallas as pl
from jax.experimental.pallas import tpu as pltpu
from jax.sharding import PartitionSpec as P

EXPERTS = 4
LANES = 128
LAG = 1
MESH = pl.DeviceIdType.MESH
BF16 = jnp.bfloat16
F32 = jnp.float32


def kernel(
    dims,
    dtab,
    ctab,
    wtab,
    tok,
    gain,
    wg_hbm,
    wu_hbm,
    wd_hbm,
    out,
    wgu,
    wd,
    arows,
    rrows,
    disp,
    xbuf,
    normed,
    stage,
    psend,
    precv,
    rsend,
    tall,
    xmat,
    gu,
    hid,
    summed,
    w_sem,
    disp_sem,
    init_sem,
    a_sem,
    relay_send,
    relay_recv,
    pair_send,
    pair_recv,
    rs_send,
    rs_recv,
    x_send,
    x_recv,
    st_send,
    st_recv,
):
    micros, depth, layers, zsize, cap, sub = dims
    toks = tok.shape[1]
    group = zsize * cap
    ff = wg_hbm.shape[2]
    sec = lax.axis_index("section")
    g = lax.axis_index("expert")
    layer = sec // 2
    col = sec % 2
    z = g // 2
    core = g % 2
    partner = 2 * z + (1 - core)
    owner = col == core
    slots = EXPERTS * cap

    def load_weights():
        return (
            pltpu.make_async_copy(wg_hbm.at[0], wgu.at[:, pl.ds(0, ff)], w_sem.at[0]),
            pltpu.make_async_copy(wu_hbm.at[0], wgu.at[:, pl.ds(ff, ff)], w_sem.at[1]),
            pltpu.make_async_copy(wd_hbm.at[0], wd, w_sem.at[2]),
        )

    for copy in load_weights():
        copy.start()

    def taken(ref, sem):
        pltpu.make_async_copy(ref, ref, sem).wait()

    def normalize(rows, gain_row):
        wide = rows.astype(F32)
        square = jnp.sum(wide * wide, axis=2, keepdims=True)
        square = jnp.sum(square, axis=1, keepdims=True)
        scale = lax.rsqrt(square * (1.0 / depth) + 1e-05)
        normed[...] = (wide * scale * gain_row[None]).astype(BF16)

    def spread(m, table, slot, send_sem, next_layer, may_self):
        for q in range(slots):
            disp[slot, q] = normed[dtab[table + m * slots + q]]

        def one(i, carry):
            to_col = i // zsize
            to_z = (z + i) % zsize
            expert = 2 * to_col + to_z // (zsize // 2)
            src = disp.at[slot, pl.ds(expert * cap, cap)]
            dst = arows.at[m, core, pl.ds(z * cap, cap)]

            def remote():
                pltpu.make_async_remote_copy(
                    src_ref=src,
                    dst_ref=dst,
                    send_sem=send_sem.at[m],
                    recv_sem=a_sem.at[m],
                    device_id=(2 * next_layer + to_col, 2 * to_z + core),
                    device_id_type=MESH,
                ).start()

            if may_self:
                here = (to_col == col) & (to_z == z)

                @pl.when(here)
                def _():
                    pltpu.make_async_copy(src, dst, a_sem.at[m]).start()

                @pl.when(jnp.logical_not(here))
                def _():
                    remote()
            else:
                remote()
            return carry

        lax.fori_loop(0, 2 * zsize, one, 0)

    def enter(m):
        normalize(tok[m], gain[0])
        spread(m, micros * slots, micros + m, init_sem, 0, True)

    def x_copy(m):
        return pltpu.make_async_remote_copy(
            src_ref=stage.at[m, 1],
            dst_ref=xbuf.at[m],
            send_sem=x_send.at[m],
            recv_sem=x_recv.at[m],
            device_id=(sec + 2, g),
            device_id_type=MESH,
        )

    def state_copy(m):
        return pltpu.make_async_remote_copy(
            src_ref=stage.at[m, 1 - core],
            dst_ref=out.at[m],
            send_sem=st_send.at[m],
            recv_sem=st_recv.at[m],
            device_id=(2 * layer + 1 - core, g),
            device_id_type=MESH,
        )

    def relay_copy(m):
        return pltpu.make_async_remote_copy(
            src_ref=arows.at[m, core],
            dst_ref=arows.at[m, core],
            send_sem=relay_send.at[m],
            recv_sem=relay_recv.at[m],
            device_id=(sec, partner),
            device_id_type=MESH,
        )

    def pair_copy(m):
        return pltpu.make_async_remote_copy(
            src_ref=psend.at[m],
            dst_ref=precv.at[m],
            send_sem=pair_send.at[m],
            recv_sem=pair_recv.at[m],
            device_id=(sec, partner),
            device_id_type=MESH,
        )

    def experts(m):
        taken(arows.at[m, core], a_sem.at[m])
        relay_copy(m).start()

        @pl.when(m == 0)
        def _():
            for copy in load_weights():
                copy.wait()

        taken(arows.at[m, 1 - core], relay_recv.at[m])
        tall[...] = arows[m].reshape(2 * group * sub, LANES).astype(F32)
        for k in range(sub):
            xmat[:, k * LANES : (k + 1) * LANES] = tall[
                pl.ds(k, 2 * group, stride=sub), :
            ].astype(BF16)
        width = 2 * LANES
        for n in range(2 * ff // width):
            cols = slice(n * width, (n + 1) * width)
            gu[:, cols] = jnp.dot(xmat[...], wgu[:, cols], preferred_element_type=F32)
        gate = gu[:, :ff]
        hid[...] = (gate / (1.0 + jnp.exp(-gate)) * gu[:, ff:]).astype(BF16)
        for n in range(depth // width):
            part = jnp.dot(
                hid[...], wd[:, n * width : (n + 1) * width], preferred_element_type=F32
            )
            for k in range(2):
                tall[pl.ds(2 * n + k, 2 * group, stride=sub), :] = part[
                    :, k * LANES : (k + 1) * LANES
                ]
        away = pl.multiple_of((1 - core) * group * sub, group * sub)
        home = pl.multiple_of(core * group * sub, group * sub)
        psend[m] = tall[pl.ds(away, group * sub), :].astype(BF16).reshape(group, sub, LANES)
        pair_copy(m).start()
        taken(precv.at[m], pair_recv.at[m])
        mine = tall[pl.ds(home, group * sub), :].reshape(group, sub, LANES)
        rsend[m] = (mine + precv[m].astype(F32)).astype(BF16)

        def one(i, carry):
            to_z = (z + i) % zsize
            src = rsend.at[m, pl.ds(to_z * cap, cap)]
            dst = rrows.at[m, pl.ds((col * zsize + z) * cap, cap)]
            here = owner & (to_z == z)

            @pl.when(here)
            def _():
                pltpu.make_async_copy(src, dst, rs_recv.at[m]).start()

            @pl.when(jnp.logical_not(here))
            def _():
                pltpu.make_async_remote_copy(
                    src_ref=src,
                    dst_ref=dst,
                    send_sem=rs_send.at[m],
                    recv_sem=rs_recv.at[m],
                    device_id=(2 * layer + core, 2 * to_z + core),
                    device_id_type=MESH,
                ).start()

            return carry

        lax.fori_loop(0, zsize, one, 0)

    def combine(m):
        taken(rrows.at[m], rs_recv.at[m])

        @pl.when(layer > 0)
        def _():
            taken(xbuf.at[m], x_recv.at[m])

        for e in range(EXPERTS):
            first = e * (zsize // 2) * cap
            total = rrows[m, first : first + cap].astype(F32)
            for b in range(1, zsize // 2):
                start = first + b * cap
                total = total + rrows[m, start : start + cap].astype(F32)
            summed[e * cap : (e + 1) * cap] = total.astype(BF16).astype(F32)
        for t in range(toks):
            wide = xbuf[m, t].astype(F32)
            at = (m * toks + t) * 2
            chosen = [summed[ctab[at + k]] for k in range(2)]
            far = micros * toks * 2
            half = wide + wtab[at] * chosen[0] + wtab[at + 1] * chosen[1]
            full = half + wtab[far + at] * chosen[0] + wtab[far + at + 1] * chosen[1]
            stage[m, 0, t] = half.astype(BF16)
            stage[m, 1, t] = full.astype(BF16)

        @pl.when(layer < layers - 1)
        def _():
            normalize(stage[m, 1], gain[jnp.minimum(layer + 1, layers - 1)])
            spread(m, 0, m, disp_sem, layer + 1, False)
            x_copy(m).start()

        state_copy(m).start()
        out[m] = stage[m, core]

    entering = owner & (layer == 0)

    @pl.when(entering)
    def _():
        xbuf[...] = tok[...]
        enter(0)

    def step(i, carry):
        @pl.when(entering & (i + 1 < micros))
        def _():
            enter(i + 1)

        @pl.when(i < micros)
        def _():
            experts(i)

        @pl.when(owner & (i >= LAG))
        def _():
            combine(i - LAG)

        return carry

    lax.fori_loop(0, micros + LAG, step, 0)

    def finish(m, carry):
        relay_copy(m).wait_send()
        pair_copy(m).wait_send()

        @pl.when(owner)
        def _():
            taken(rsend.at[m, pl.ds(0, group - cap)], rs_send.at[m])
            state_copy(m).wait_send()

            @pl.when(layer < layers - 1)
            def _():
                taken(rrows.at[m], disp_sem.at[m])
                x_copy(m).wait_send()

        @pl.when(jnp.logical_not(owner))
        def _():
            taken(rsend.at[m], rs_send.at[m])
            state_copy(m).wait_recv()

        @pl.when(entering)
        def _():
            taken(rrows.at[m, pl.ds(0, 2 * group - cap)], init_sem.at[m])

        return carry

    lax.fori_loop(0, micros, finish, 0)


def on_device(tokens, norm_gain, w_gate, w_up, w_down, expert_ids, slot_ids, dropped, gate_weights):
    micros, toks, depth = tokens.shape
    layers = norm_gain.shape[0]
    ff = w_gate.shape[2]
    zsize = lax.axis_size("expert") // 2
    cap = 5 * toks // (2 * EXPERTS)
    sub = depth // LANES
    group = zsize * cap
    layer = lax.axis_index("section") // 2
    slots = EXPERTS * cap

    def at_layer(value, index):
        return lax.dynamic_index_in_dim(value, index, 0, keepdims=False)

    key_all = jnp.where(dropped == 0, expert_ids * cap + slot_ids, -1)
    keys = jnp.stack([at_layer(key_all, jnp.minimum(layer + 1, layers - 1)), key_all[0]])
    token_at = jnp.arange(toks, dtype=jnp.int32)[:, None, None]
    hits = keys[..., None] == jnp.arange(slots, dtype=jnp.int32)
    dtab = jnp.sum(jnp.where(hits, token_at, 0), axis=(2, 3)).reshape(-1)
    ids = at_layer(expert_ids, layer)
    ctab = (ids * cap + at_layer(slot_ids, layer)).reshape(-1)
    weigh = jnp.where(at_layer(dropped, layer) == 0, at_layer(gate_weights, layer), 0.0)
    first = ids < EXPERTS // 2
    wtab = jnp.stack([jnp.where(first, weigh, 0.0), jnp.where(first, 0.0, weigh)]).reshape(-1)

    smem = pl.BlockSpec(memory_space=pltpu.SMEM)
    vmem = pl.BlockSpec(memory_space=pltpu.VMEM)
    hbm = pl.BlockSpec(memory_space=pl.ANY)
    tile = (sub, LANES)
    dma = pltpu.SemaphoreType.DMA
    states = pl.pallas_call(
        functools.partial(kernel, (micros, depth, layers, zsize, cap, sub)),
        out_shape=jax.ShapeDtypeStruct((micros, toks) + tile, BF16),
        in_specs=[smem, smem, smem, vmem, vmem, hbm, hbm, hbm],
        out_specs=vmem,
        scratch_shapes=[
            pltpu.VMEM((depth, 2 * ff), BF16),
            pltpu.VMEM((ff, depth), BF16),
            pltpu.VMEM((micros, 2, group) + tile, BF16),
            pltpu.VMEM((micros, 2 * group) + tile, BF16),
            pltpu.VMEM((2 * micros, slots) + tile, BF16),
            pltpu.VMEM((micros, toks) + tile, BF16),
            pltpu.VMEM((toks,) + tile, BF16),
            pltpu.VMEM((micros, 2, toks) + tile, BF16),
            pltpu.VMEM((micros, group) + tile, BF16),
            pltpu.VMEM((micros, group) + tile, BF16),
            pltpu.VMEM((micros, group) + tile, BF16),
            pltpu.VMEM((2 * group * sub, LANES), F32),
            pltpu.VMEM((2 * group, depth), BF16),
            pltpu.VMEM((2 * group, 2 * ff), F32),
            pltpu.VMEM((2 * group, ff), BF16),
            pltpu.VMEM((slots,) + tile, F32),
            dma((3,)),
        ]
        + [dma((micros,))] * 13,
        compiler_params=pltpu.CompilerParams(
            has_side_effects=True, vmem_limit_bytes=60 * 1024 * 1024
        ),
    )(
        dtab,
        ctab,
        wtab,
        tokens.reshape((micros, toks) + tile),
        norm_gain.reshape((layers,) + tile),
        w_gate,
        w_up,
        w_down,
    )
    return states.reshape(1, micros, toks, depth)


def solution(mesh):
    return jax.shard_map(
        on_device,
        mesh=mesh,
        in_specs=(
            P(None, "expert", None),
            P(),
            P("section", None, "expert"),
            P("section", None, "expert"),
            P("section", "expert", None),
            P(None, None, "expert", None),
            P(None, None, "expert", None),
            P(None, None, "expert", None),
            P(None, None, "expert", None),
        ),
        out_specs=P("section", None, "expert", None),
        check_vma=False,
    )
```

```python
import functools

import jax
import jax.numpy as jnp
from jax import lax
from jax.experimental import pallas as pl
from jax.experimental.pallas import tpu as pltpu
from jax.sharding import PartitionSpec as P

EXPERTS = 4
LANES = 128
MESH = pl.DeviceIdType.MESH
BF16 = jnp.bfloat16
F32 = jnp.float32


def kernel(
    dims,
    dtab,
    ctab,
    wfirst,
    wsecond,
    tok,
    gain,
    wg_hbm,
    wu_hbm,
    wd_hbm,
    out,
    wgu,
    wd,
    arows,
    rrows,
    disp,
    xbuf,
    normed,
    stage,
    psend,
    precv,
    rsend,
    tall,
    xmat,
    gu,
    hid,
    summed,
    states,
    gains,
    w_sem,
    disp_sem,
    init_sem,
    a_sem,
    relay_send,
    relay_recv,
    pair_send,
    pair_recv,
    rs_send,
    rs_recv,
    x_send,
    x_recv,
    st_send,
    st_recv,
):
    micros, depth, layers, zsize, cap, sub = dims
    toks = tok.shape[0] // micros
    group = zsize * cap
    ff = wg_hbm.shape[2]
    sec = lax.axis_index("section")
    g = lax.axis_index("expert")
    layer = sec // 2
    col = sec % 2
    z = g // 2
    core = g % 2
    partner = 2 * z + (1 - core)
    owner = col == core
    slots = EXPERTS * cap

    def load_weights():
        return (
            pltpu.make_async_copy(wg_hbm.at[0], wgu.at[:, pl.ds(0, ff)], w_sem.at[0]),
            pltpu.make_async_copy(wu_hbm.at[0], wgu.at[:, pl.ds(ff, ff)], w_sem.at[1]),
            pltpu.make_async_copy(wd_hbm.at[0], wd, w_sem.at[2]),
        )

    for copy in load_weights():
        copy.start()

    def far_first(i):
        return (z + zsize // 2 - (i + 1) // 2 * (2 * (i % 2) - 1)) % zsize

    def taken(ref, sem):
        pltpu.make_async_copy(ref, ref, sem).wait()

    def normalize(rows, gain_row):
        wide = rows.astype(F32)
        square = jnp.sum(wide * wide, axis=2, keepdims=True)
        square = jnp.sum(square, axis=1, keepdims=True)
        scale = lax.rsqrt(square * (1.0 / depth) + 1e-05)
        normed[...] = (wide * scale * gain_row[None]).astype(BF16)

    def spread(m, table, slot, send_sem, next_layer, may_self):
        for q in range(slots):
            disp[slot, q] = normed[dtab[table, m, q]]

        def one(i, carry):
            to_col = i % 2
            to_z = far_first(i // 2)
            expert = 2 * to_col + to_z // (zsize // 2)
            src = disp.at[slot, pl.ds(expert * cap, cap)]
            dst = arows.at[m, core, pl.ds(z * cap, cap)]

            def remote():
                pltpu.make_async_remote_copy(
                    src_ref=src,
                    dst_ref=dst,
                    send_sem=send_sem.at[m],
                    recv_sem=a_sem.at[m],
                    device_id=(2 * next_layer + to_col, 2 * to_z + core),
                    device_id_type=MESH,
                ).start()

            if may_self:
                here = (to_col == col) & (to_z == z)

                @pl.when(here)
                def _():
                    pltpu.make_async_copy(src, dst, a_sem.at[m]).start()

                @pl.when(jnp.logical_not(here))
                def _():
                    remote()
            else:
                remote()
            return carry

        lax.fori_loop(0, 2 * zsize, one, 0)

    def enter(m):
        normalize(xbuf[m], gains[0])
        spread(m, 1, micros + m, init_sem, 0, True)

    def x_copy(m):
        return pltpu.make_async_remote_copy(
            src_ref=stage.at[m, 1],
            dst_ref=xbuf.at[m],
            send_sem=x_send.at[m],
            recv_sem=x_recv.at[m],
            device_id=(sec + 2, g),
            device_id_type=MESH,
        )

    def state_copy(m):
        return pltpu.make_async_remote_copy(
            src_ref=stage.at[m, 1 - core],
            dst_ref=states.at[m],
            send_sem=st_send.at[m],
            recv_sem=st_recv.at[m],
            device_id=(2 * layer + 1 - core, g),
            device_id_type=MESH,
        )

    def relay_copy(m):
        return pltpu.make_async_remote_copy(
            src_ref=arows.at[m, core],
            dst_ref=arows.at[m, core],
            send_sem=relay_send.at[m],
            recv_sem=relay_recv.at[m],
            device_id=(sec, partner),
            device_id_type=MESH,
        )

    def pair_copy(m):
        return pltpu.make_async_remote_copy(
            src_ref=psend.at[m],
            dst_ref=precv.at[m],
            send_sem=pair_send.at[m],
            recv_sem=pair_recv.at[m],
            device_id=(sec, partner),
            device_id_type=MESH,
        )

    def experts(m):
        def place(part):
            at = pl.multiple_of(part * group * sub, group * sub)
            wide = arows[m, part].reshape(group * sub, LANES).astype(F32)
            tall[pl.ds(at, group * sub), :] = wide

        taken(arows.at[m, core], a_sem.at[m])
        relay_copy(m).start()

        @pl.when(m == 0)
        def _():
            for copy in load_weights():
                copy.wait()

        place(core)
        taken(arows.at[m, 1 - core], relay_recv.at[m])
        place(1 - core)
        for k in range(sub):
            xmat[:, k * LANES : (k + 1) * LANES] = tall[
                pl.ds(k, 2 * group, stride=sub), :
            ].astype(BF16)
        width = ff
        for n in range(2 * ff // width):
            cols = slice(n * width, (n + 1) * width)
            gu[:, cols] = jnp.dot(xmat[...], wgu[:, cols], preferred_element_type=F32)
        gate = gu[:, :ff]
        hid[...] = (gate / (1.0 + jnp.exp(-gate)) * gu[:, ff:]).astype(BF16)
        width = min(depth, 8 * LANES)
        for n in range(depth // width):
            part = jnp.dot(
                hid[...], wd[:, n * width : (n + 1) * width], preferred_element_type=F32
            )
            for k in range(width // LANES):
                tall[pl.ds(width // LANES * n + k, 2 * group, stride=sub), :] = part[
                    :, k * LANES : (k + 1) * LANES
                ]
        away = pl.multiple_of((1 - core) * group * sub, group * sub)
        home = pl.multiple_of(core * group * sub, group * sub)
        psend[m] = tall[pl.ds(away, group * sub), :].astype(BF16).reshape(group, sub, LANES)
        pair_copy(m).start()
        taken(precv.at[m], pair_recv.at[m])
        mine = tall[pl.ds(home, group * sub), :].reshape(group, sub, LANES)
        rsend[m] = (mine + precv[m].astype(F32)).astype(BF16)

        def one(i, carry):
            to_z = far_first(i)
            src = rsend.at[m, pl.ds(to_z * cap, cap)]
            dst = rrows.at[m, pl.ds((col * zsize + z) * cap, cap)]
            here = owner & (to_z == z)

            @pl.when(here)
            def _():
                pltpu.make_async_copy(src, dst, rs_recv.at[m]).start()

            @pl.when(jnp.logical_not(here))
            def _():
                pltpu.make_async_remote_copy(
                    src_ref=src,
                    dst_ref=dst,
                    send_sem=rs_send.at[m],
                    recv_sem=rs_recv.at[m],
                    device_id=(2 * layer + core, 2 * to_z + core),
                    device_id_type=MESH,
                ).start()

            return carry

        lax.fori_loop(0, zsize, one, 0)

    def combine(m):
        taken(rrows.at[m], rs_recv.at[m])

        @pl.when(layer > 0)
        def _():
            taken(xbuf.at[m], x_recv.at[m])

        for e in range(EXPERTS):
            first = e * (zsize // 2) * cap
            total = rrows[m, first : first + cap].astype(F32)
            for b in range(1, zsize // 2):
                start = first + b * cap
                total = total + rrows[m, start : start + cap].astype(F32)
            summed[e * cap : (e + 1) * cap] = total.astype(BF16).astype(F32)
        for t in range(toks):
            wide = xbuf[m, t].astype(F32)
            chosen = [summed[ctab[m, k, t]] for k in range(2)]
            half = wide + wfirst[m, 0, t] * chosen[0] + wfirst[m, 1, t] * chosen[1]
            full = half + wsecond[m, 0, t] * chosen[0] + wsecond[m, 1, t] * chosen[1]
            stage[m, 0, t] = half.astype(BF16)
            stage[m, 1, t] = full.astype(BF16)

        @pl.when(layer < layers - 1)
        def _():
            normalize(stage[m, 1], gains[1])
            spread(m, 0, m, disp_sem, layer + 1, False)
            x_copy(m).start()

        state_copy(m).start()
        states[m] = stage[m, core]

    entering = owner & (layer == 0)
    later = gain[pl.ds(jnp.minimum(layer + 1, layers - 1), 1), :]
    for k in range(sub):
        cols = slice(k * LANES, (k + 1) * LANES)
        gains[0, k : k + 1, :] = gain[0:1, cols]
        gains[1, k : k + 1, :] = later[:, cols]

    @pl.when(entering)
    def _():
        rows = micros * toks
        for k in range(sub):
            tall[pl.ds(k, rows, stride=sub), :] = tok[:, k * LANES : (k + 1) * LANES].astype(F32)
        flat = tall[pl.ds(0, rows * sub), :].astype(BF16)
        xbuf[...] = flat.reshape(micros, toks, sub, LANES)
        enter(0)

    def step(i, carry):
        @pl.when(entering & (i + 1 < micros))
        def _():
            enter(i + 1)

        experts(i)

        @pl.when(owner)
        def _():
            combine(i)

        return carry

    lax.fori_loop(0, micros, step, 0)

    def finish(m, carry):
        relay_copy(m).wait_send()
        pair_copy(m).wait_send()

        @pl.when(owner)
        def _():
            taken(rsend.at[m, pl.ds(0, group - cap)], rs_send.at[m])
            state_copy(m).wait_send()

            @pl.when(layer < layers - 1)
            def _():
                taken(rrows.at[m], disp_sem.at[m])
                x_copy(m).wait_send()

        @pl.when(jnp.logical_not(owner))
        def _():
            taken(rsend.at[m], rs_send.at[m])
            state_copy(m).wait_recv()

        @pl.when(entering)
        def _():
            taken(rrows.at[m, pl.ds(0, 2 * group - cap)], init_sem.at[m])

        return carry

    lax.fori_loop(0, micros, finish, 0)
    rows = micros * toks
    tall[pl.ds(0, rows * sub), :] = states[...].reshape(rows * sub, LANES).astype(F32)
    for k in range(sub):
        out[:, k * LANES : (k + 1) * LANES] = tall[pl.ds(k, rows, stride=sub), :].astype(BF16)


def on_device(tokens, norm_gain, w_gate, w_up, w_down, expert_ids, slot_ids, dropped, gate_weights):
    micros, toks, depth = tokens.shape
    layers = norm_gain.shape[0]
    ff = w_gate.shape[2]
    zsize = lax.axis_size("expert") // 2
    cap = 5 * toks // (2 * EXPERTS)
    sub = depth // LANES
    group = zsize * cap
    layer = lax.axis_index("section") // 2
    slots = EXPERTS * cap

    def at_layer(value, index):
        return lax.dynamic_index_in_dim(value, index, 0, keepdims=False)

    key_all = jnp.where(dropped == 0, expert_ids * cap + slot_ids, -1)
    keys = jnp.stack([at_layer(key_all, jnp.minimum(layer + 1, layers - 1)), key_all[0]])
    token_at = jnp.arange(toks, dtype=jnp.int32)[:, None, None]
    hits = keys[..., None] == jnp.arange(slots, dtype=jnp.int32)
    dtab = jnp.sum(jnp.where(hits, token_at, 0), axis=(2, 3))
    ids = at_layer(expert_ids, layer)
    ctab = (ids * cap + at_layer(slot_ids, layer)).swapaxes(1, 2)
    weigh = jnp.where(at_layer(dropped, layer) == 0, at_layer(gate_weights, layer), 0.0)
    wfirst = jnp.where(ids < EXPERTS // 2, weigh, 0.0).swapaxes(1, 2)
    wsecond = jnp.where(ids < EXPERTS // 2, 0.0, weigh).swapaxes(1, 2)

    smem = pl.BlockSpec(memory_space=pltpu.SMEM)
    vmem = pl.BlockSpec(memory_space=pltpu.VMEM)
    hbm = pl.BlockSpec(memory_space=pl.ANY)
    tile = (sub, LANES)
    dma = pltpu.SemaphoreType.DMA
    states = pl.pallas_call(
        functools.partial(kernel, (micros, depth, layers, zsize, cap, sub)),
        out_shape=jax.ShapeDtypeStruct((micros * toks, depth), BF16),
        in_specs=[smem, smem, smem, smem, vmem, vmem, hbm, hbm, hbm],
        out_specs=vmem,
        scratch_shapes=[
            pltpu.VMEM((depth, 2 * ff), BF16),
            pltpu.VMEM((ff, depth), BF16),
            pltpu.VMEM((micros, 2, group) + tile, BF16),
            pltpu.VMEM((micros, 2 * group) + tile, BF16),
            pltpu.VMEM((2 * micros, slots) + tile, BF16),
            pltpu.VMEM((micros, toks) + tile, BF16),
            pltpu.VMEM((toks,) + tile, BF16),
            pltpu.VMEM((micros, 2, toks) + tile, BF16),
            pltpu.VMEM((micros, group) + tile, BF16),
            pltpu.VMEM((micros, group) + tile, BF16),
            pltpu.VMEM((micros, group) + tile, BF16),
            pltpu.VMEM((max(2 * group, micros * toks) * sub, LANES), F32),
            pltpu.VMEM((2 * group, depth), BF16),
            pltpu.VMEM((2 * group, 2 * ff), F32),
            pltpu.VMEM((2 * group, ff), BF16),
            pltpu.VMEM((slots,) + tile, F32),
            pltpu.VMEM((micros, toks) + tile, BF16),
            pltpu.VMEM((2,) + tile, F32),
            dma((3,)),
        ]
        + [dma((micros,))] * 13,
        compiler_params=pltpu.CompilerParams(
            has_side_effects=True, vmem_limit_bytes=60 * 1024 * 1024
        ),
    )(
        dtab,
        ctab,
        wfirst,
        wsecond,
        tokens.reshape(micros * toks, depth),
        norm_gain,
        w_gate,
        w_up,
        w_down,
    )
    return states.reshape(1, micros, toks, depth)


def solution(mesh):
    return jax.shard_map(
        on_device,
        mesh=mesh,
        in_specs=(
            P(None, "expert", None),
            P(),
            P("section", None, "expert"),
            P("section", None, "expert"),
            P("section", "expert", None),
            P(None, None, "expert", None),
            P(None, None, "expert", None),
            P(None, None, "expert", None),
            P(None, None, "expert", None),
        ),
        out_specs=P("section", None, "expert", None),
        check_vma=False,
    )
```

```python
import functools

import jax
import jax.numpy as jnp
from jax import lax
from jax.experimental import pallas as pl
from jax.experimental.pallas import tpu as pltpu
from jax.sharding import PartitionSpec as P

EXPERTS = 4
LANES = 128
MESH = pl.DeviceIdType.MESH
BF16 = jnp.bfloat16
F32 = jnp.float32


def kernel(
    dims,
    dtab,
    ctab,
    wfirst,
    wsecond,
    tok,
    gain,
    wg_hbm,
    wu_hbm,
    wd_hbm,
    out,
    wgu,
    wd,
    arows,
    rrows,
    disp,
    xbuf,
    normed,
    stage,
    psend,
    precv,
    rsend,
    tall,
    xmat,
    gu,
    hid,
    summed,
    states,
    gains,
    w_sem,
    disp_sem,
    init_sem,
    a_sem,
    relay_send,
    relay_recv,
    pair_send,
    pair_recv,
    rs_send,
    rs_recv,
    x_send,
    x_recv,
    st_send,
    st_recv,
):
    micros, depth, layers, zsize, cap, sub = dims
    toks = tok.shape[0] // micros
    group = zsize * cap
    ff = wg_hbm.shape[2]
    sec = lax.axis_index("section")
    g = lax.axis_index("expert")
    layer = sec // 2
    col = sec % 2
    z = g // 2
    core = g % 2
    partner = 2 * z + (1 - core)
    owner = col == core
    slots = EXPERTS * cap

    def load_weights():
        return (
            pltpu.make_async_copy(wg_hbm.at[0], wgu.at[:, pl.ds(0, ff)], w_sem.at[0]),
            pltpu.make_async_copy(wu_hbm.at[0], wgu.at[:, pl.ds(ff, ff)], w_sem.at[1]),
            pltpu.make_async_copy(wd_hbm.at[0], wd, w_sem.at[2]),
        )

    for copy in load_weights():
        copy.start()

    def greet(section, index):
        pl.semaphore_signal(
            pltpu.get_barrier_semaphore(),
            inc=1,
            device_id=(section, index),
            device_id_type=MESH,
        )

    def greet_plane(section):
        def one(i, carry):
            @pl.when((section != sec) | (i != z))
            def _():
                greet(section, 2 * i + core)

            return carry

        lax.fori_loop(0, zsize, one, 0)

    greet(sec, partner)

    @pl.when(owner)
    def _():
        greet_plane(2 * layer)
        greet_plane(2 * layer + 1)

    @pl.when(jnp.logical_not(owner) & (layer == 0))
    def _():
        greet_plane(core)

    @pl.when(layer > 0)
    def _():
        greet_plane(2 * (layer - 1) + core)

    @pl.when(jnp.logical_not(owner) & (layer > 0))
    def _():
        greet(2 * layer + core, g)

    own_greets = jnp.where(layer == 0, 2 * zsize, zsize + 1)
    next_greets = jnp.where(layer < layers - 1, 2 * zsize, 0)
    greets = jnp.where(owner, own_greets + next_greets, 1 + zsize)

    def far_first(i):
        return (z + zsize // 2 - (i + 1) // 2 * (2 * (i % 2) - 1)) % zsize

    def taken(ref, sem):
        pltpu.make_async_copy(ref, ref, sem).wait()

    def normalize(rows, gain_row):
        wide = rows.astype(F32)
        square = jnp.sum(wide * wide, axis=2, keepdims=True)
        square = jnp.sum(square, axis=1, keepdims=True)
        scale = lax.rsqrt(square * (1.0 / depth) + 1e-05)
        normed[...] = (wide * scale * gain_row[None]).astype(BF16)

    def spread(m, table, slot, send_sem, next_layer, may_self):
        for q in range(slots):
            disp[slot, q] = normed[dtab[table, m, q]]

        def one(i, carry):
            to_col = i % 2
            to_z = far_first(i // 2)
            expert = 2 * to_col + to_z // (zsize // 2)
            src = disp.at[slot, pl.ds(expert * cap, cap)]
            dst = arows.at[m, core, pl.ds(z * cap, cap)]

            def remote():
                pltpu.make_async_remote_copy(
                    src_ref=src,
                    dst_ref=dst,
                    send_sem=send_sem.at[m],
                    recv_sem=a_sem.at[m],
                    device_id=(2 * next_layer + to_col, 2 * to_z + core),
                    device_id_type=MESH,
                ).start()

            if may_self:
                here = (to_col == col) & (to_z == z)

                @pl.when(here)
                def _():
                    pltpu.make_async_copy(src, dst, a_sem.at[m]).start()

                @pl.when(jnp.logical_not(here))
                def _():
                    remote()
            else:
                remote()
            return carry

        lax.fori_loop(0, 2 * zsize, one, 0)

    def enter(m):
        normalize(xbuf[m], gains[0])
        spread(m, 1, micros + m, init_sem, 0, True)

    def x_copy(m):
        return pltpu.make_async_remote_copy(
            src_ref=stage.at[m, 1],
            dst_ref=xbuf.at[m],
            send_sem=x_send.at[m],
            recv_sem=x_recv.at[m],
            device_id=(sec + 2, g),
            device_id_type=MESH,
        )

    def state_copy(m):
        return pltpu.make_async_remote_copy(
            src_ref=stage.at[m, 1 - core],
            dst_ref=states.at[m],
            send_sem=st_send.at[m],
            recv_sem=st_recv.at[m],
            device_id=(2 * layer + 1 - core, g),
            device_id_type=MESH,
        )

    def relay_copy(m):
        return pltpu.make_async_remote_copy(
            src_ref=arows.at[m, core],
            dst_ref=arows.at[m, core],
            send_sem=relay_send.at[m],
            recv_sem=relay_recv.at[m],
            device_id=(sec, partner),
            device_id_type=MESH,
        )

    def pair_copy(m):
        return pltpu.make_async_remote_copy(
            src_ref=psend.at[m],
            dst_ref=precv.at[m],
            send_sem=pair_send.at[m],
            recv_sem=pair_recv.at[m],
            device_id=(sec, partner),
            device_id_type=MESH,
        )

    def experts(m):
        def place(part):
            at = pl.multiple_of(part * group * sub, group * sub)
            wide = arows[m, part].reshape(group * sub, LANES).astype(F32)
            tall[pl.ds(at, group * sub), :] = wide

        taken(arows.at[m, core], a_sem.at[m])
        relay_copy(m).start()

        @pl.when(m == 0)
        def _():
            for copy in load_weights():
                copy.wait()

        place(core)
        taken(arows.at[m, 1 - core], relay_recv.at[m])
        place(1 - core)
        for k in range(sub):
            xmat[:, k * LANES : (k + 1) * LANES] = tall[
                pl.ds(k, 2 * group, stride=sub), :
            ].astype(BF16)
        width = ff
        for n in range(2 * ff // width):
            cols = slice(n * width, (n + 1) * width)
            gu[:, cols] = jnp.dot(xmat[...], wgu[:, cols], preferred_element_type=F32)
        gate = gu[:, :ff]
        hid[...] = (gate / (1.0 + jnp.exp(-gate)) * gu[:, ff:]).astype(BF16)
        width = min(depth, 8 * LANES)
        for n in range(depth // width):
            part = jnp.dot(
                hid[...], wd[:, n * width : (n + 1) * width], preferred_element_type=F32
            )
            for k in range(width // LANES):
                tall[pl.ds(width // LANES * n + k, 2 * group, stride=sub), :] = part[
                    :, k * LANES : (k + 1) * LANES
                ]
        away = pl.multiple_of((1 - core) * group * sub, group * sub)
        home = pl.multiple_of(core * group * sub, group * sub)
        psend[m] = tall[pl.ds(away, group * sub), :].astype(BF16).reshape(group, sub, LANES)
        pair_copy(m).start()
        taken(precv.at[m], pair_recv.at[m])
        mine = tall[pl.ds(home, group * sub), :].reshape(group, sub, LANES)
        rsend[m] = (mine + precv[m].astype(F32)).astype(BF16)

        def one(i, carry):
            to_z = far_first(i)
            src = rsend.at[m, pl.ds(to_z * cap, cap)]
            dst = rrows.at[m, pl.ds((col * zsize + z) * cap, cap)]
            here = owner & (to_z == z)

            @pl.when(here)
            def _():
                pltpu.make_async_copy(src, dst, rs_recv.at[m]).start()

            @pl.when(jnp.logical_not(here))
            def _():
                pltpu.make_async_remote_copy(
                    src_ref=src,
                    dst_ref=dst,
                    send_sem=rs_send.at[m],
                    recv_sem=rs_recv.at[m],
                    device_id=(2 * layer + core, 2 * to_z + core),
                    device_id_type=MESH,
                ).start()

            return carry

        lax.fori_loop(0, zsize, one, 0)

    def combine(m):
        taken(rrows.at[m], rs_recv.at[m])

        @pl.when(layer > 0)
        def _():
            taken(xbuf.at[m], x_recv.at[m])

        for e in range(EXPERTS):
            first = e * (zsize // 2) * cap
            total = rrows[m, first : first + cap].astype(F32)
            for b in range(1, zsize // 2):
                start = first + b * cap
                total = total + rrows[m, start : start + cap].astype(F32)
            summed[e * cap : (e + 1) * cap] = total.astype(BF16).astype(F32)
        for t in range(toks):
            wide = xbuf[m, t].astype(F32)
            chosen = [summed[ctab[m, k, t]] for k in range(2)]
            half = wide + wfirst[m, 0, t] * chosen[0] + wfirst[m, 1, t] * chosen[1]
            full = half + wsecond[m, 0, t] * chosen[0] + wsecond[m, 1, t] * chosen[1]
            stage[m, 0, t] = half.astype(BF16)
            stage[m, 1, t] = full.astype(BF16)

        @pl.when(layer < layers - 1)
        def _():
            normalize(stage[m, 1], gains[1])
            spread(m, 0, m, disp_sem, layer + 1, False)
            x_copy(m).start()

        state_copy(m).start()
        states[m] = stage[m, core]

    pl.semaphore_wait(pltpu.get_barrier_semaphore(), greets)
    entering = owner & (layer == 0)
    later = gain[pl.ds(jnp.minimum(layer + 1, layers - 1), 1), :]
    for k in range(sub):
        cols = slice(k * LANES, (k + 1) * LANES)
        gains[0, k : k + 1, :] = gain[0:1, cols]
        gains[1, k : k + 1, :] = later[:, cols]

    @pl.when(entering)
    def _():
        rows = micros * toks
        for k in range(sub):
            tall[pl.ds(k, rows, stride=sub), :] = tok[:, k * LANES : (k + 1) * LANES].astype(F32)
        flat = tall[pl.ds(0, rows * sub), :].astype(BF16)
        xbuf[...] = flat.reshape(micros, toks, sub, LANES)
        enter(0)

    def step(i, carry):
        @pl.when(entering & (i + 1 < micros))
        def _():
            enter(i + 1)

        experts(i)

        @pl.when(owner)
        def _():
            combine(i)

        return carry

    lax.fori_loop(0, micros, step, 0)

    def finish(m, carry):
        relay_copy(m).wait_send()
        pair_copy(m).wait_send()

        @pl.when(owner)
        def _():
            taken(rsend.at[m, pl.ds(0, group - cap)], rs_send.at[m])
            state_copy(m).wait_send()

            @pl.when(layer < layers - 1)
            def _():
                taken(rrows.at[m], disp_sem.at[m])
                x_copy(m).wait_send()

        @pl.when(jnp.logical_not(owner))
        def _():
            taken(rsend.at[m], rs_send.at[m])
            state_copy(m).wait_recv()

        @pl.when(entering)
        def _():
            taken(rrows.at[m, pl.ds(0, 2 * group - cap)], init_sem.at[m])

        return carry

    lax.fori_loop(0, micros, finish, 0)
    rows = micros * toks
    tall[pl.ds(0, rows * sub), :] = states[...].reshape(rows * sub, LANES).astype(F32)
    for k in range(sub):
        out[:, k * LANES : (k + 1) * LANES] = tall[pl.ds(k, rows, stride=sub), :].astype(BF16)


def on_device(tokens, norm_gain, w_gate, w_up, w_down, expert_ids, slot_ids, dropped, gate_weights):
    micros, toks, depth = tokens.shape
    layers = norm_gain.shape[0]
    ff = w_gate.shape[2]
    zsize = lax.axis_size("expert") // 2
    cap = 5 * toks // (2 * EXPERTS)
    sub = depth // LANES
    group = zsize * cap
    layer = lax.axis_index("section") // 2
    slots = EXPERTS * cap

    def at_layer(value, index):
        return lax.dynamic_index_in_dim(value, index, 0, keepdims=False)

    key_all = jnp.where(dropped == 0, expert_ids * cap + slot_ids, -1)
    keys = jnp.stack([at_layer(key_all, jnp.minimum(layer + 1, layers - 1)), key_all[0]])
    token_at = jnp.arange(toks, dtype=jnp.int32)[:, None, None]
    hits = keys[..., None] == jnp.arange(slots, dtype=jnp.int32)
    dtab = jnp.sum(jnp.where(hits, token_at, 0), axis=(2, 3))
    ids = at_layer(expert_ids, layer)
    ctab = (ids * cap + at_layer(slot_ids, layer)).swapaxes(1, 2)
    weigh = jnp.where(at_layer(dropped, layer) == 0, at_layer(gate_weights, layer), 0.0)
    wfirst = jnp.where(ids < EXPERTS // 2, weigh, 0.0).swapaxes(1, 2)
    wsecond = jnp.where(ids < EXPERTS // 2, 0.0, weigh).swapaxes(1, 2)

    smem = pl.BlockSpec(memory_space=pltpu.SMEM)
    vmem = pl.BlockSpec(memory_space=pltpu.VMEM)
    hbm = pl.BlockSpec(memory_space=pl.ANY)
    tile = (sub, LANES)
    dma = pltpu.SemaphoreType.DMA
    states = pl.pallas_call(
        functools.partial(kernel, (micros, depth, layers, zsize, cap, sub)),
        out_shape=jax.ShapeDtypeStruct((micros * toks, depth), BF16),
        in_specs=[smem, smem, smem, smem, vmem, vmem, hbm, hbm, hbm],
        out_specs=vmem,
        scratch_shapes=[
            pltpu.VMEM((depth, 2 * ff), BF16),
            pltpu.VMEM((ff, depth), BF16),
            pltpu.VMEM((micros, 2, group) + tile, BF16),
            pltpu.VMEM((micros, 2 * group) + tile, BF16),
            pltpu.VMEM((2 * micros, slots) + tile, BF16),
            pltpu.VMEM((micros, toks) + tile, BF16),
            pltpu.VMEM((toks,) + tile, BF16),
            pltpu.VMEM((micros, 2, toks) + tile, BF16),
            pltpu.VMEM((micros, group) + tile, BF16),
            pltpu.VMEM((micros, group) + tile, BF16),
            pltpu.VMEM((micros, group) + tile, BF16),
            pltpu.VMEM((max(2 * group, micros * toks) * sub, LANES), F32),
            pltpu.VMEM((2 * group, depth), BF16),
            pltpu.VMEM((2 * group, 2 * ff), F32),
            pltpu.VMEM((2 * group, ff), BF16),
            pltpu.VMEM((slots,) + tile, F32),
            pltpu.VMEM((micros, toks) + tile, BF16),
            pltpu.VMEM((2,) + tile, F32),
            dma((3,)),
        ]
        + [dma((micros,))] * 13,
        compiler_params=pltpu.CompilerParams(
            collective_id=0, has_side_effects=True, vmem_limit_bytes=60 * 1024 * 1024
        ),
    )(
        dtab,
        ctab,
        wfirst,
        wsecond,
        tokens.reshape(micros * toks, depth),
        norm_gain,
        w_gate,
        w_up,
        w_down,
    )
    return states.reshape(1, micros, toks, depth)


def solution(mesh):
    return jax.shard_map(
        on_device,
        mesh=mesh,
        in_specs=(
            P(None, "expert", None),
            P(),
            P("section", None, "expert"),
            P("section", None, "expert"),
            P("section", "expert", None),
            P(None, None, "expert", None),
            P(None, None, "expert", None),
            P(None, None, "expert", None),
            P(None, None, "expert", None),
        ),
        out_specs=P("section", None, "expert", None),
        check_vma=False,
    )
```

```python
import functools

import jax
import jax.numpy as jnp
from jax import lax
from jax.experimental import pallas as pl
from jax.experimental.pallas import tpu as pltpu
from jax.sharding import PartitionSpec as P

EXPERTS = 4
LANES = 128
MESH = pl.DeviceIdType.MESH
BF16 = jnp.bfloat16
F32 = jnp.float32


def kernel(
    dims,
    dtab,
    ctab,
    wfirst,
    wsecond,
    tok,
    gain,
    wg_hbm,
    wu_hbm,
    wd_hbm,
    out,
    wgu,
    wd,
    arows,
    rrows,
    disp,
    xbuf,
    normed,
    stage,
    psend,
    precv,
    rsend,
    tall,
    xmat,
    gu,
    hid,
    summed,
    states,
    gains,
    w_sem,
    disp_sem,
    init_sem,
    a_sem,
    relay_send,
    relay_recv,
    pair_send,
    pair_recv,
    rs_send,
    rs_recv,
    x_send,
    x_recv,
    st_send,
    st_recv,
):
    micros, depth, layers, zsize, cap, sub = dims
    toks = tok.shape[0] // micros
    group = zsize * cap
    ff = wg_hbm.shape[2]
    sec = lax.axis_index("section")
    g = lax.axis_index("expert")
    layer = sec // 2
    col = sec % 2
    z = g // 2
    core = g % 2
    partner = 2 * z + (1 - core)
    owner = col == core
    slots = EXPERTS * cap

    def load_weights():
        return (
            pltpu.make_async_copy(wg_hbm.at[0], wgu.at[:, pl.ds(0, ff)], w_sem.at[0]),
            pltpu.make_async_copy(wu_hbm.at[0], wgu.at[:, pl.ds(ff, ff)], w_sem.at[1]),
            pltpu.make_async_copy(wd_hbm.at[0], wd, w_sem.at[2]),
        )

    for copy in load_weights():
        copy.start()

    def greet(section, index):
        pl.semaphore_signal(
            pltpu.get_barrier_semaphore(),
            inc=1,
            device_id=(section, index),
            device_id_type=MESH,
        )

    def greet_plane(section):
        def one(i, carry):
            @pl.when((section != sec) | (i != z))
            def _():
                greet(section, 2 * i + core)

            return carry

        lax.fori_loop(0, zsize, one, 0)

    greet(sec, partner)

    @pl.when(owner)
    def _():
        greet_plane(2 * layer)
        greet_plane(2 * layer + 1)

    @pl.when(jnp.logical_not(owner) & (layer == 0))
    def _():
        greet_plane(core)

    @pl.when(layer > 0)
    def _():
        greet_plane(2 * (layer - 1) + core)

    @pl.when(jnp.logical_not(owner) & (layer > 0))
    def _():
        greet(2 * layer + core, g)

    own_greets = jnp.where(layer == 0, 2 * zsize, zsize + 1)
    next_greets = jnp.where(layer < layers - 1, 2 * zsize, 0)
    greets = jnp.where(owner, own_greets + next_greets, 1 + zsize)

    def far_first(i):
        return (z + zsize // 2 - (i + 1) // 2 * (2 * (i % 2) - 1)) % zsize

    def taken(ref, sem):
        pltpu.make_async_copy(ref, ref, sem).wait()

    def normalize(rows, gain_row):
        wide = rows.astype(F32)
        square = jnp.sum(wide * wide, axis=2, keepdims=True)
        square = jnp.sum(square, axis=1, keepdims=True)
        scale = lax.rsqrt(square * (1.0 / depth) + 1e-05)
        normed[...] = (wide * scale * gain_row[None]).astype(BF16)

    def spread(m, table, slot, send_sem, next_layer, may_self):
        for q in range(slots):
            disp[slot, q] = normed[dtab[table, m, q]]

        def one(i, carry):
            to_col = i % 2
            to_z = far_first(i // 2)
            expert = 2 * to_col + to_z // (zsize // 2)
            src = disp.at[slot, pl.ds(expert * cap, cap)]
            dst = arows.at[m, core, pl.ds(z * cap, cap)]

            def remote():
                pltpu.make_async_remote_copy(
                    src_ref=src,
                    dst_ref=dst,
                    send_sem=send_sem.at[m],
                    recv_sem=a_sem.at[m],
                    device_id=(2 * next_layer + to_col, 2 * to_z + core),
                    device_id_type=MESH,
                ).start()

            if may_self:
                here = (to_col == col) & (to_z == z)

                @pl.when(here)
                def _():
                    pltpu.make_async_copy(src, dst, a_sem.at[m]).start()

                @pl.when(jnp.logical_not(here))
                def _():
                    remote()
            else:
                remote()
            return carry

        lax.fori_loop(0, 2 * zsize, one, 0)

    def enter(m):
        normalize(xbuf[m], gains[0])
        spread(m, 1, micros + m, init_sem, 0, True)

    def x_copy(m):
        return pltpu.make_async_remote_copy(
            src_ref=stage.at[m, 1],
            dst_ref=xbuf.at[m],
            send_sem=x_send.at[m],
            recv_sem=x_recv.at[m],
            device_id=(sec + 2, g),
            device_id_type=MESH,
        )

    def state_copy(m):
        return pltpu.make_async_remote_copy(
            src_ref=stage.at[m, 1 - core],
            dst_ref=states.at[m],
            send_sem=st_send.at[m],
            recv_sem=st_recv.at[m],
            device_id=(2 * layer + 1 - core, g),
            device_id_type=MESH,
        )

    def relay_copy(m):
        return pltpu.make_async_remote_copy(
            src_ref=arows.at[m, core],
            dst_ref=arows.at[m, core],
            send_sem=relay_send.at[m],
            recv_sem=relay_recv.at[m],
            device_id=(sec, partner),
            device_id_type=MESH,
        )

    def pair_copy(m):
        return pltpu.make_async_remote_copy(
            src_ref=psend.at[m],
            dst_ref=precv.at[m],
            send_sem=pair_send.at[m],
            recv_sem=pair_recv.at[m],
            device_id=(sec, partner),
            device_id_type=MESH,
        )

    def experts(m):
        def place(part):
            at = pl.multiple_of(part * group * sub, group * sub)
            wide = arows[m, part].reshape(group * sub, LANES).astype(F32)
            tall[pl.ds(at, group * sub), :] = wide

        taken(arows.at[m, core], a_sem.at[m])
        relay_copy(m).start()

        @pl.when(m == 0)
        def _():
            for copy in load_weights()[:2]:
                copy.wait()

        place(core)
        taken(arows.at[m, 1 - core], relay_recv.at[m])
        place(1 - core)
        for k in range(sub):
            xmat[:, k * LANES : (k + 1) * LANES] = tall[
                pl.ds(k, 2 * group, stride=sub), :
            ].astype(BF16)
        width = ff
        for n in range(2 * ff // width):
            cols = slice(n * width, (n + 1) * width)
            gu[:, cols] = jnp.dot(xmat[...], wgu[:, cols], preferred_element_type=F32)
        gate = gu[:, :ff]
        hid[...] = (gate / (1.0 + jnp.exp(-gate)) * gu[:, ff:]).astype(BF16)

        @pl.when(m == 0)
        def _():
            load_weights()[2].wait()

        width = min(depth, 8 * LANES)
        for n in range(depth // width):
            part = jnp.dot(
                hid[...], wd[:, n * width : (n + 1) * width], preferred_element_type=F32
            )
            for k in range(width // LANES):
                tall[pl.ds(width // LANES * n + k, 2 * group, stride=sub), :] = part[
                    :, k * LANES : (k + 1) * LANES
                ]
        away = pl.multiple_of((1 - core) * group * sub, group * sub)
        home = pl.multiple_of(core * group * sub, group * sub)
        psend[m] = tall[pl.ds(away, group * sub), :].astype(BF16).reshape(group, sub, LANES)
        pair_copy(m).start()
        taken(precv.at[m], pair_recv.at[m])
        mine = tall[pl.ds(home, group * sub), :].reshape(group, sub, LANES)
        rsend[m] = (mine + precv[m].astype(F32)).astype(BF16)

        def one(i, carry):
            to_z = far_first(i)
            src = rsend.at[m, pl.ds(to_z * cap, cap)]
            dst = rrows.at[m, pl.ds((col * zsize + z) * cap, cap)]
            here = owner & (to_z == z)

            @pl.when(here)
            def _():
                pltpu.make_async_copy(src, dst, rs_recv.at[m]).start()

            @pl.when(jnp.logical_not(here))
            def _():
                pltpu.make_async_remote_copy(
                    src_ref=src,
                    dst_ref=dst,
                    send_sem=rs_send.at[m],
                    recv_sem=rs_recv.at[m],
                    device_id=(2 * layer + core, 2 * to_z + core),
                    device_id_type=MESH,
                ).start()

            return carry

        lax.fori_loop(0, zsize, one, 0)

    def combine(m):
        taken(rrows.at[m], rs_recv.at[m])

        @pl.when(layer > 0)
        def _():
            taken(xbuf.at[m], x_recv.at[m])

        for e in range(EXPERTS):
            first = e * (zsize // 2) * cap
            total = rrows[m, first : first + cap].astype(F32)
            for b in range(1, zsize // 2):
                start = first + b * cap
                total = total + rrows[m, start : start + cap].astype(F32)
            summed[e * cap : (e + 1) * cap] = total.astype(BF16).astype(F32)
        for t in range(toks):
            wide = xbuf[m, t].astype(F32)
            chosen = [summed[ctab[m, k, t]] for k in range(2)]
            half = wide + wfirst[m, 0, t] * chosen[0] + wfirst[m, 1, t] * chosen[1]
            full = half + wsecond[m, 0, t] * chosen[0] + wsecond[m, 1, t] * chosen[1]
            stage[m, 0, t] = half.astype(BF16)
            stage[m, 1, t] = full.astype(BF16)

        @pl.when(layer < layers - 1)
        def _():
            normalize(stage[m, 1], gains[1])
            spread(m, 0, m, disp_sem, layer + 1, False)
            x_copy(m).start()

        state_copy(m).start()
        states[m] = stage[m, core]

    entering = owner & (layer == 0)
    later = gain[pl.ds(jnp.minimum(layer + 1, layers - 1), 1), :]
    for k in range(sub):
        cols = slice(k * LANES, (k + 1) * LANES)
        gains[0, k : k + 1, :] = gain[0:1, cols]
        gains[1, k : k + 1, :] = later[:, cols]

    @pl.when(entering)
    def _():
        rows = micros * toks
        for k in range(sub):
            tall[pl.ds(k, rows, stride=sub), :] = tok[:, k * LANES : (k + 1) * LANES].astype(F32)
        flat = tall[pl.ds(0, rows * sub), :].astype(BF16)
        xbuf[...] = flat.reshape(micros, toks, sub, LANES)

    pl.semaphore_wait(pltpu.get_barrier_semaphore(), greets)

    @pl.when(entering)
    def _():
        enter(0)

    def step(i, carry):
        @pl.when(entering & (i + 1 < micros))
        def _():
            enter(i + 1)

        experts(i)

        @pl.when(owner)
        def _():
            combine(i)

        return carry

    lax.fori_loop(0, micros, step, 0)

    def finish(m, carry):
        relay_copy(m).wait_send()
        pair_copy(m).wait_send()

        @pl.when(owner)
        def _():
            taken(rsend.at[m, pl.ds(0, group - cap)], rs_send.at[m])
            state_copy(m).wait_send()

            @pl.when(layer < layers - 1)
            def _():
                taken(rrows.at[m], disp_sem.at[m])
                x_copy(m).wait_send()

        @pl.when(jnp.logical_not(owner))
        def _():
            taken(rsend.at[m], rs_send.at[m])
            state_copy(m).wait_recv()

        @pl.when(entering)
        def _():
            taken(rrows.at[m, pl.ds(0, 2 * group - cap)], init_sem.at[m])

        return carry

    lax.fori_loop(0, micros, finish, 0)
    rows = micros * toks
    tall[pl.ds(0, rows * sub), :] = states[...].reshape(rows * sub, LANES).astype(F32)
    for k in range(sub):
        out[:, k * LANES : (k + 1) * LANES] = tall[pl.ds(k, rows, stride=sub), :].astype(BF16)


def on_device(tokens, norm_gain, w_gate, w_up, w_down, expert_ids, slot_ids, dropped, gate_weights):
    micros, toks, depth = tokens.shape
    layers = norm_gain.shape[0]
    ff = w_gate.shape[2]
    zsize = lax.axis_size("expert") // 2
    cap = 5 * toks // (2 * EXPERTS)
    sub = depth // LANES
    group = zsize * cap
    layer = lax.axis_index("section") // 2
    slots = EXPERTS * cap

    def at_layer(value, index):
        return lax.dynamic_index_in_dim(value, index, 0, keepdims=False)

    key_all = jnp.where(dropped == 0, expert_ids * cap + slot_ids, -1)
    keys = jnp.stack([at_layer(key_all, jnp.minimum(layer + 1, layers - 1)), key_all[0]])
    token_at = jnp.arange(toks, dtype=jnp.int32)[:, None, None]
    hits = keys[..., None] == jnp.arange(slots, dtype=jnp.int32)
    dtab = jnp.sum(jnp.where(hits, token_at, 0), axis=(2, 3))
    ids = at_layer(expert_ids, layer)
    ctab = (ids * cap + at_layer(slot_ids, layer)).swapaxes(1, 2)
    weigh = jnp.where(at_layer(dropped, layer) == 0, at_layer(gate_weights, layer), 0.0)
    wfirst = jnp.where(ids < EXPERTS // 2, weigh, 0.0).swapaxes(1, 2)
    wsecond = jnp.where(ids < EXPERTS // 2, 0.0, weigh).swapaxes(1, 2)

    smem = pl.BlockSpec(memory_space=pltpu.SMEM)
    vmem = pl.BlockSpec(memory_space=pltpu.VMEM)
    hbm = pl.BlockSpec(memory_space=pl.ANY)
    tile = (sub, LANES)
    dma = pltpu.SemaphoreType.DMA
    states = pl.pallas_call(
        functools.partial(kernel, (micros, depth, layers, zsize, cap, sub)),
        out_shape=jax.ShapeDtypeStruct((micros * toks, depth), BF16),
        in_specs=[smem, smem, smem, smem, vmem, vmem, hbm, hbm, hbm],
        out_specs=vmem,
        scratch_shapes=[
            pltpu.VMEM((depth, 2 * ff), BF16),
            pltpu.VMEM((ff, depth), BF16),
            pltpu.VMEM((micros, 2, group) + tile, BF16),
            pltpu.VMEM((micros, 2 * group) + tile, BF16),
            pltpu.VMEM((2 * micros, slots) + tile, BF16),
            pltpu.VMEM((micros, toks) + tile, BF16),
            pltpu.VMEM((toks,) + tile, BF16),
            pltpu.VMEM((micros, 2, toks) + tile, BF16),
            pltpu.VMEM((micros, group) + tile, BF16),
            pltpu.VMEM((micros, group) + tile, BF16),
            pltpu.VMEM((micros, group) + tile, BF16),
            pltpu.VMEM((max(2 * group, micros * toks) * sub, LANES), F32),
            pltpu.VMEM((2 * group, depth), BF16),
            pltpu.VMEM((2 * group, 2 * ff), F32),
            pltpu.VMEM((2 * group, ff), BF16),
            pltpu.VMEM((slots,) + tile, F32),
            pltpu.VMEM((micros, toks) + tile, BF16),
            pltpu.VMEM((2,) + tile, F32),
            dma((3,)),
        ]
        + [dma((micros,))] * 13,
        compiler_params=pltpu.CompilerParams(
            collective_id=0, has_side_effects=True, vmem_limit_bytes=60 * 1024 * 1024
        ),
    )(
        dtab,
        ctab,
        wfirst,
        wsecond,
        tokens.reshape(micros * toks, depth),
        norm_gain,
        w_gate,
        w_up,
        w_down,
    )
    return states.reshape(1, micros, toks, depth)


def solution(mesh):
    return jax.shard_map(
        on_device,
        mesh=mesh,
        in_specs=(
            P(None, "expert", None),
            P(),
            P("section", None, "expert"),
            P("section", None, "expert"),
            P("section", "expert", None),
            P(None, None, "expert", None),
            P(None, None, "expert", None),
            P(None, None, "expert", None),
            P(None, None, "expert", None),
        ),
        out_specs=P("section", None, "expert", None),
        check_vma=False,
    )
```
